512 devices in a mesh: ka: 128 (over y, x_hi, z), col: 4 (over x_lo, core).
Axes of the slice: x: 4 (x_hi: 2, x_lo: 2; x = x_hi * 2 + x_lo), y: 4, z: 16, core: 2. Of those that a mesh axis runs over, the one named last changes fastest.
Arguments:
- amps: bfloat16 [256, 256, 192], P('ka', 'col'), may hold values from -6 to 6
- isdf_coeffs: bfloat16 [256, 2048, 256], P('ka', 'col'), may hold values from -0.375 to 0.375
- w_screen: bfloat16 [16, 2048, 2048], P(None, 'ka', 'col'), as said below
- energies: float32 [256, 256], P('ka', 'col'), may hold values from 0.5 to 3
- qsel: int32 [2], replicated, may hold values from 0 to 15
- partner: int32 [2, 256], replicated, may hold values from 0 to 255, each once within a row
Outputs:
- applied: float32 [256, 256, 192], P('ka', 'col')
The draws below stay inside these ranges and needn't reach their ends.
Inputs may be any that keep to these rules, and one draw needn't show every extreme that they name: Each row of partner is a permutation of the 256 k points. `w_screen`: each of the 16 matrices is symmetric.
All inputs are finite; a program needn't handle non-finite values.
Results may differ from the reference program's by a relative error of at most 0.013.
Values may be sent and summed in bfloat16 or wider, within the bound.
No kernel may reach another device: no remote copies, remote signals or barrier semaphores. Data moves between devices by JAX's collectives and lax.ppermute only.
A program may use at most 64 MiB of HBM per device.

```python
import math
import jax
import jax.numpy as jnp
from jax import lax

NMU = 2048
NPAIR = 256
NEXC = 192
NQW = 16
NK = 256
N_COL = 4


def draw_w_screen(key, part):
    normals = jax.random.normal(jax.random.fold_in(key, 11), (NQW, NMU, NMU), jnp.float32)
    matrix = (normals + jnp.swapaxes(normals, 1, 2)) * (0.6 / (2.0 * NMU) ** 0.5)
    return matrix.astype(jnp.bfloat16)


def block_scale(own_key, dims, pieces, least, largest):
    def one(axis_at, blocks):
        heights = jax.random.uniform(jax.random.fold_in(jax.random.fold_in(own_key, 6), axis_at), (blocks,), jnp.float32, least / len(pieces), largest / len(pieces))
        return jnp.repeat(jnp.exp(heights), dims[axis_at] // blocks).reshape((-1,) + (1,) * (len(dims) - axis_at - 1))

    loudness = one(*pieces[0])
    for cut in pieces[1:]:
        loudness = loudness * one(*cut)
    return loudness


def noise(stream_key, shape, deviation, most, cuts=(), held_as=jnp.bfloat16):
    values = deviation * jax.random.normal(stream_key, shape, jnp.float32)
    if cuts:
        values = values * block_scale(stream_key, shape, cuts, -0.22, 0.18)
    return jnp.clip(values, -most, most).astype(held_as)


def setup_inputs(seed: int = 0) -> dict:
    streams_of = jax.random.split(jax.random.key(seed), 7)
    amps = noise(streams_of[0], (NK, NPAIR, NEXC), 1.0, 6.0, ((0, 128), (1, 4)))
    isdf_coeffs = noise(streams_of[1], (NK, NMU, NPAIR), NPAIR ** -0.5, 0.375, ((0, 128), (1, 4)))
    w_screen = draw_w_screen(jax.random.fold_in(streams_of[6], 71), 0)
    energies = jnp.clip(jnp.exp(math.log(3.0) - 1.7917595 * jax.random.uniform(streams_of[3], (NK, NPAIR), jnp.float32) ** block_scale(streams_of[3], (NK, NPAIR), ((0, 128), (1, 4)), -0.2, 0.2)), 0.5, 3.0)
    qsel = jax.random.randint(streams_of[4], (2,), 0, NQW).astype(jnp.int32)
    partner = jax.vmap(lambda own: jax.random.permutation(own, NK))(jax.random.split(streams_of[5], 2)).reshape((2, NK)).astype(jnp.int32)
    return dict(amps=amps, isdf_coeffs=isdf_coeffs, w_screen=w_screen, energies=energies, qsel=qsel, partner=partner)


def reference(amps, isdf_coeffs, w_screen, energies, qsel, partner):
    high = lax.Precision.HIGHEST
    block_rows = NMU // N_COL
    screens = [jnp.take(w_screen, qsel[shift], axis=0).astype(jnp.float32) for shift in range(2)]

    def per_point(index):
        coeffs_k = isdf_coeffs[index].astype(jnp.float32)
        total = energies[index][:, None] * amps[index].astype(jnp.float32)
        for shift in range(2):
            partner_amps = jnp.take(amps, partner[shift, index], axis=0).astype(jnp.float32)
            densities = jnp.dot(coeffs_k, partner_amps, precision=high).astype(jnp.bfloat16).astype(jnp.float32)
            screened = jnp.zeros((NMU, NEXC), jnp.float32)
            for block in range(N_COL):
                lower = block * block_rows
                upper = lower + block_rows
                partial_part = jnp.dot(screens[shift][:, lower:upper], densities[lower:upper], precision=high)
                partial_part = lax.optimization_barrier(partial_part.astype(jnp.bfloat16)).astype(jnp.float32)
                screened = screened + partial_part
            screened = screened.astype(jnp.bfloat16).astype(jnp.float32)
            total = total + jnp.dot(coeffs_k.T, screened, precision=high)
        return total

    return lax.map(per_point, jnp.arange(NK, dtype=jnp.int32))
```

```python
import jax
import jax.numpy as jnp
from jax import lax
from jax.experimental import pallas as pl
from jax.experimental.pallas import tpu as pltpu
from jax.sharding import Mesh
from jax.sharding import PartitionSpec as P

KA = ("y", "xh", "z")
COL = ("xl", "c")
PLANE = ("y", "xh")
N_Y, N_XH, N_Z, N_COL = 4, 2, 16, 4
VEC = 192
SMEM = pl.BlockSpec(memory_space=pltpu.SMEM)
VMEM = pl.BlockSpec(memory_space=pltpu.VMEM)


def send_kernel(partner, place, line, out):
    z = place[1]
    for yx in range(N_Y * N_XH):
        for slot in range(4):
            wanted = partner[slot // 2, 2 * (yx * N_Z + z) + slot % 2]
            out[yx, slot] = line[wanted & 31]


def keep_kernel(partner, place, arrived, out):
    own = 2 * (place[0] * N_Z + place[1])
    for slot in range(4):
        wanted = partner[slot // 2, own + slot % 2]
        out[slot] = arrived[wanted >> 5, slot]


def by_z(block):
    rows = [block[(xh * N_Z + z) * 16 : (xh * N_Z + z + 1) * 16] for z in range(N_Z) for xh in range(N_XH)]
    return jnp.concatenate(rows, axis=0)


def density_kernel(partners, *refs):
    pieces, out = refs[:-1], refs[-1]
    turned = []
    for slot in range(4):
        whole = jnp.concatenate([partners[c, slot] for c in range(N_COL)], axis=0)
        turned.append(whole.astype(jnp.float32).T.astype(jnp.bfloat16))
    for kl in range(2):
        vectors = jnp.concatenate([turned[kl], turned[2 + kl]], axis=0)
        for i, piece in enumerate(pieces):
            dens = lax.dot_general(
                vectors, by_z(piece[kl]), (((1,), (1,)), ((), ())), preferred_element_type=jnp.float32
            ).astype(jnp.bfloat16)
            out[i, 0, kl * VEC : (kl + 1) * VEC, :] = dens[:VEC]
            out[i, 1, kl * VEC : (kl + 1) * VEC, :] = dens[VEC:]


def screen_kernel(place, w, dens, coeffs, out):
    c = place[2]
    screened = []
    for j in range(2):
        total = None
        for i in range(N_COL):
            rows = w[:, c ^ i, j].reshape(512, 512)
            part = jnp.dot(dens[i, j], rows, preferred_element_type=jnp.float32)
            total = part if total is None else total + part
        screened.append(total.astype(jnp.bfloat16))
    for kl in range(2):
        own = slice(kl * VEC, (kl + 1) * VEC)
        projected = jnp.dot(screened[0][own], coeffs[kl], preferred_element_type=jnp.float32)
        projected += jnp.dot(screened[1][own], coeffs[kl], preferred_element_type=jnp.float32)
        result = projected.T.astype(jnp.bfloat16)
        for dest in range(N_COL):
            out[dest, kl] = result[dest * 64 : (dest + 1) * 64]


def swapped(array, axis):
    return lax.ppermute(array, axis, [(0, 1), (1, 0)])


def call(kernel, shape, *args):
    specs = [SMEM if a.dtype == jnp.int32 else VMEM for a in args]
    return pl.pallas_call(
        kernel, out_shape=jax.ShapeDtypeStruct(shape, jnp.bfloat16), in_specs=specs, out_specs=VMEM
    )(*args)


def body(amps, isdf_coeffs, w_screen, energies, qsel, partner):
    place = jnp.stack([lax.axis_index(PLANE), lax.axis_index("z"), lax.axis_index(COL)]).astype(jnp.int32)
    slabs = jnp.stack([lax.dynamic_index_in_dim(w_screen, qsel[j], 0, keepdims=False) for j in range(2)])
    pair = lax.all_gather(slabs, "xh", axis=1, tiled=True)
    plane = lax.all_gather(pair, "y", axis=0, tiled=False)
    plane, amps_, coeffs_ = lax.optimization_barrier((plane, amps, isdf_coeffs))
    rows = lax.all_gather(plane, "z", axis=0, tiled=False)

    from_core = swapped(coeffs_, "c")
    from_x = swapped(coeffs_, "xl")
    from_both = swapped(from_x, "c")

    line = lax.all_gather(amps_, "z", axis=0, tiled=True)
    send = call(send_kernel, (8, 4, 64, VEC), partner, place, line)
    arrived = lax.all_to_all(send, PLANE, 0, 0, tiled=True)
    kept = call(keep_kernel, (4, 64, VEC), partner, place, arrived)
    partners = lax.all_gather(kept, COL, axis=0, tiled=False)

    dens = call(density_kernel, (4, 2, 2 * VEC, 512), partners, isdf_coeffs, from_core, from_x, from_both)
    projected = call(screen_kernel, (N_COL, 2, 64, VEC), place, rows, dens, isdf_coeffs)
    summed = lax.all_to_all(projected, COL, 0, 0, tiled=True).astype(jnp.float32).sum(axis=0)
    return summed + energies[:, :, None] * amps.astype(jnp.float32)


def solution(mesh):
    torus = Mesh(mesh.devices.reshape(N_Y, N_XH, N_Z, 2, 2), KA + COL)
    placed = (P(KA, COL, None), P(KA, COL, None), P(None, KA, COL), P(KA, COL), P(), P())
    return jax.shard_map(body, mesh=torus, in_specs=placed, out_specs=P(KA, COL, None), check_vma=False)
```

```python
import jax
import jax.numpy as jnp
from jax import lax
from jax.experimental import pallas as pl
from jax.experimental.pallas import tpu as pltpu
from jax.sharding import Mesh
from jax.sharding import PartitionSpec as P

KA = ("y", "xh", "z")
COL = ("xl", "c")
PLANE = ("y", "xh")
N_Y, N_XH, N_Z, N_COL = 4, 2, 16, 4
VEC = 192
SMEM = pl.BlockSpec(memory_space=pltpu.SMEM)
VMEM = pl.BlockSpec(memory_space=pltpu.VMEM)
HBM = pl.BlockSpec(memory_space=pltpu.HBM)


def slab_kernel(qsel, w, out, arrived):
    copies = [pltpu.make_async_copy(w.at[qsel[j]], out.at[j], arrived.at[j]) for j in range(2)]
    for copy in copies:
        copy.start()
    for copy in copies:
        copy.wait()


def send_kernel(partner, line, out):
    z = lax.axis_index("z")
    for yx in range(N_Y * N_XH):
        for slot in range(4):
            wanted = partner[slot // 2, 2 * (yx * N_Z + z) + slot % 2]
            out[yx, slot] = line[wanted & 31]


def keep_kernel(partner, arrived, out):
    own = 2 * (lax.axis_index(PLANE) * N_Z + lax.axis_index("z"))
    for slot in range(4):
        wanted = partner[slot // 2, own + slot % 2]
        out[slot] = arrived[wanted >> 5, slot]


def by_z(block):
    rows = [block[(xh * N_Z + z) * 16 : (xh * N_Z + z + 1) * 16] for z in range(N_Z) for xh in range(N_XH)]
    return jnp.concatenate(rows, axis=0)


def density_kernel(partners, *refs):
    pieces, (out, coeffs, arrived) = refs[:N_COL], refs[N_COL:]
    copies = [pltpu.make_async_copy(pieces[i], coeffs.at[i], arrived.at[i]) for i in range(N_COL)]
    for copy in copies:
        copy.start()
    turned = []
    for slot in range(4):
        whole = jnp.concatenate([partners[c, slot] for c in range(N_COL)], axis=0)
        turned.append(whole.astype(jnp.float32).T.astype(jnp.bfloat16))
    vectors = [jnp.concatenate([turned[kl], turned[2 + kl]], axis=0) for kl in range(2)]
    for i in range(N_COL):
        copies[i].wait()
        for kl in range(2):
            dens = lax.dot_general(
                vectors[kl], by_z(coeffs[i, kl]), (((1,), (1,)), ((), ())), preferred_element_type=jnp.float32
            ).astype(jnp.bfloat16)
            out[i, 0, kl * VEC : (kl + 1) * VEC, :] = dens[:VEC]
            out[i, 1, kl * VEC : (kl + 1) * VEC, :] = dens[VEC:]


def screen_kernel(w, dens, own_coeffs, out, rows, coeffs, arrived, ready):
    c = lax.axis_index(COL)
    copies = [
        [pltpu.make_async_copy(w.at[:, c ^ i, j], rows.at[i, j], arrived.at[i, j]) for i in range(N_COL)]
        for j in range(2)
    ]
    for j in range(2):
        for i in range(N_COL):
            copies[j][i].start()
    last = pltpu.make_async_copy(own_coeffs, coeffs, ready)
    last.start()
    screened = []
    for j in range(2):
        total = None
        for i in range(N_COL):
            copies[j][i].wait()
            part = jnp.dot(dens[i, j], rows[i, j].reshape(512, 512), preferred_element_type=jnp.float32)
            total = part if total is None else total + part
        screened.append(total.astype(jnp.bfloat16))
    last.wait()
    for kl in range(2):
        own = slice(kl * VEC, (kl + 1) * VEC)
        projected = jnp.dot(screened[0][own], coeffs[kl], preferred_element_type=jnp.float32)
        projected += jnp.dot(screened[1][own], coeffs[kl], preferred_element_type=jnp.float32)
        result = projected.T.astype(jnp.bfloat16)
        for dest in range(N_COL):
            out[dest, kl] = result[dest * 64 : (dest + 1) * 64]


def swapped(array, axis):
    return lax.ppermute(array, axis, [(0, 1), (1, 0)])


def call(kernel, shape, specs, mib, *args, scratch=()):
    return pl.pallas_call(
        kernel,
        out_shape=jax.ShapeDtypeStruct(shape, jnp.bfloat16),
        in_specs=specs,
        out_specs=VMEM,
        scratch_shapes=scratch,
        compiler_params=pltpu.CompilerParams(vmem_limit_bytes=mib << 20),
    )(*args)


def sent_to_all(array, axis):
    length = lax.axis_size(axis)
    return lax.all_to_all(jnp.broadcast_to(array[None], (length, *array.shape)), axis, 0, 0, tiled=True)


def body(amps, isdf_coeffs, w_screen, energies, qsel, partner):
    slabs = call(
        slab_kernel, (2, 16, 512), [SMEM, HBM], 2, qsel, w_screen, scratch=[pltpu.SemaphoreType.DMA((2,))]
    )
    plane = sent_to_all(slabs, PLANE).reshape(N_Y, N_XH, 2, 16, 512).transpose(0, 2, 1, 3, 4)
    plane, amps_, coeffs_ = lax.optimization_barrier((plane, amps, isdf_coeffs))
    rows = lax.all_gather(plane.reshape(N_Y, 2, 32, 512), "z", axis=0, tiled=False)

    line = sent_to_all(amps_, "z").reshape(2 * N_Z, 64, VEC)
    from_core = swapped(coeffs_, "c")
    from_x = swapped(coeffs_, "xl")
    from_both = swapped(from_x, "c")

    send = call(send_kernel, (8, 4, 64, VEC), [SMEM, VMEM], 4, partner, line)
    arrived = lax.all_to_all(send, PLANE, 0, 0, tiled=True)
    kept = call(keep_kernel, (4, 64, VEC), [SMEM, VMEM], 4, partner, arrived)
    partners = lax.all_gather(kept, COL, axis=0, tiled=False)

    dens = call(
        density_kernel, (4, 2, 2 * VEC, 512), [VMEM] + [HBM] * N_COL, 56, partners, isdf_coeffs, from_core, from_x, from_both,
        scratch=[pltpu.VMEM((N_COL, 2, 512, 256), jnp.bfloat16), pltpu.SemaphoreType.DMA((N_COL,))],
    )
    projected = call(
        screen_kernel, (N_COL, 2, 64, VEC), [HBM, VMEM, HBM], 56, rows, dens, isdf_coeffs,
        scratch=[
            pltpu.VMEM((N_COL, 2, N_Z, 32, 512), jnp.bfloat16), pltpu.VMEM((2, 512, 256), jnp.bfloat16),
            pltpu.SemaphoreType.DMA((N_COL, 2)), pltpu.SemaphoreType.DMA,
        ],
    )
    summed = lax.all_to_all(projected, COL, 0, 0, tiled=True).astype(jnp.float32).sum(axis=0)
    return summed + energies[:, :, None] * amps.astype(jnp.float32)


def solution(mesh):
    torus = Mesh(mesh.devices.reshape(N_Y, N_XH, N_Z, 2, 2), KA + COL)
    placed = (P(KA, COL, None), P(KA, COL, None), P(None, KA, COL), P(KA, COL), P(), P())
    return jax.shard_map(body, mesh=torus, in_specs=placed, out_specs=P(KA, COL, None), check_vma=False)
```

```python
import jax
import jax.numpy as jnp
from jax import lax
from jax.experimental import pallas as pl
from jax.experimental.pallas import tpu as pltpu
from jax.sharding import Mesh
from jax.sharding import PartitionSpec as P


KA = ("y", "xh", "z")
COL = ("xl", "c")
PLANE = ("y", "xh")
N_Y, N_XH, N_Z, N_COL = 4, 2, 16, 4
VEC = 192
SMEM = pl.BlockSpec(memory_space=pltpu.SMEM)
VMEM = pl.BlockSpec(memory_space=pltpu.VMEM)
HBM = pl.BlockSpec(memory_space=pltpu.HBM)


def slab_kernel(qsel, w, out, arrived):
    copies = [pltpu.make_async_copy(w.at[qsel[j]], out.at[j], arrived.at[j]) for j in range(2)]
    for copy in copies:
        copy.start()
    for copy in copies:
        copy.wait()


def joined(first, second, half):
    top = lax.broadcasted_iota(jnp.int32, first.shape, 0) < 4
    return jnp.where(top, turned(first, half[0] == 1), turned(second, half[1] == 0))


def turned(tile, swap):
    other = pltpu.roll(tile, 4, 0)
    if isinstance(swap, bool):
        return other if swap else tile
    return jnp.where(swap, other, tile)


def spread_kernel(amps, out):
    for q in range(8):
        own = [amps[kl, 8 * q : 8 * q + 8].astype(jnp.float32) for kl in range(2)]
        for half in range(2):
            out[2 * q + half] = joined(own[0], own[1], (half, half)).astype(jnp.bfloat16)


def send_kernel(partner, held, out):
    base = 2 * N_Z * lax.axis_index(PLANE)
    for z in range(N_Z):
        for j in range(2):
            wanted = [partner[j, base + 2 * z + kl] for kl in range(2)]
            tiles = [held[p >> 5, (p >> 1) & 15].astype(jnp.float32) for p in wanted]
            out[z, j] = joined(tiles[0], tiles[1], (wanted[0] & 1, wanted[1] & 1)).astype(jnp.bfloat16)


def keep_kernel(arrived, out):
    for j in range(2):
        for q in range(8):
            tiles = [arrived[2 * q + half, j].astype(jnp.float32) for half in range(2)]
            for kl in range(2):
                out[2 * j + kl, 8 * q : 8 * q + 8] = joined(tiles[0], tiles[1], (kl, kl)).astype(jnp.bfloat16)


def by_z(block):
    rows = [block[(xh * N_Z + z) * 16 : (xh * N_Z + z + 1) * 16] for z in range(N_Z) for xh in range(N_XH)]
    return jnp.concatenate(rows, axis=0)


def density_kernel(partners, *refs):
    pieces, (out, coeffs, dens, arrived, written) = refs[:N_COL], refs[N_COL:]
    copies = [pltpu.make_async_copy(pieces[i], coeffs.at[i], arrived.at[i]) for i in range(N_COL)]
    stores = [pltpu.make_async_copy(dens.at[i], out.at[i], written.at[i]) for i in range(N_COL)]
    for copy in copies:
        copy.start()
    columns = []
    for slot in range(4):
        whole = jnp.concatenate([partners[c, slot] for c in range(N_COL)], axis=0)
        columns.append(whole.astype(jnp.float32).T.astype(jnp.bfloat16))
    vectors = [jnp.concatenate([columns[kl], columns[2 + kl]], axis=0) for kl in range(2)]
    for i in range(N_COL):
        copies[i].wait()
        for kl in range(2):
            part = lax.dot_general(
                vectors[kl], by_z(coeffs[i, kl]), (((1,), (1,)), ((), ())), preferred_element_type=jnp.float32
            ).astype(jnp.bfloat16)
            dens[i, 0, kl * VEC : (kl + 1) * VEC, :] = part[:VEC]
            dens[i, 1, kl * VEC : (kl + 1) * VEC, :] = part[VEC:]
        stores[i].start()
    for store in stores:
        store.wait()


def screen_kernel(w, dens, own_coeffs, out, rows, held, coeffs, arrived, fetched, ready):
    c = lax.axis_index(COL)
    steps = [(j, i) for j in range(2) for i in range(N_COL)]
    copies = {(j, i): pltpu.make_async_copy(w.at[:, c ^ i, :, j], rows.at[i, j], arrived.at[i, j]) for j, i in steps}
    fetches = {(j, i): pltpu.make_async_copy(dens.at[i, j], held.at[i, j], fetched.at[i, j]) for j, i in steps}
    for step in steps:
        fetches[step].start()
        copies[step].start()
    last = pltpu.make_async_copy(own_coeffs, coeffs, ready)
    last.start()
    screened = []
    for j in range(2):
        total = None
        for i in range(N_COL):
            fetches[j, i].wait()
            copies[j, i].wait()
            part = jnp.dot(held[i, j], rows[i, j].reshape(512, 512), preferred_element_type=jnp.float32)
            total = part if total is None else total + part
        screened.append(total.astype(jnp.bfloat16))
    last.wait()
    for kl in range(2):
        own = slice(kl * VEC, (kl + 1) * VEC)
        projected = jnp.dot(screened[0][own], coeffs[kl], preferred_element_type=jnp.float32)
        projected += jnp.dot(screened[1][own], coeffs[kl], preferred_element_type=jnp.float32)
        result = projected.T.astype(jnp.bfloat16)
        for dest in range(N_COL):
            out[dest, kl] = result[dest * 64 : (dest + 1) * 64]


def swapped(array, axis):
    return lax.ppermute(array, axis, [(0, 1), (1, 0)])


def call(kernel, shape, specs, mib, *args, scratch=(), out=VMEM):
    return pl.pallas_call(
        kernel,
        out_shape=jax.ShapeDtypeStruct(shape, jnp.bfloat16),
        in_specs=specs,
        out_specs=out,
        scratch_shapes=scratch,
        compiler_params=pltpu.CompilerParams(vmem_limit_bytes=mib << 20),
    )(*args)


def sent_to_all(array, axis):
    length = lax.axis_size(axis)
    return lax.all_to_all(jnp.broadcast_to(array[None], (length, *array.shape)), axis, 0, 0, tiled=True)


def body(amps, isdf_coeffs, w_screen, energies, qsel, partner):
    pieces = call(spread_kernel, (N_Z, 8, VEC), [VMEM], 4, amps)
    spread = lax.all_to_all(pieces, "z", 0, 0, tiled=True)
    slabs = call(
        slab_kernel, (2, 16, 512), [SMEM, HBM], 60, qsel, w_screen, scratch=[pltpu.SemaphoreType.DMA((2,))]
    )
    plane = lax.all_gather(lax.all_gather(slabs, "xh", axis=0, tiled=False), "y", axis=0, tiled=False)
    plane, coeffs = lax.optimization_barrier((plane, isdf_coeffs))
    rows = lax.all_gather(plane.reshape(N_Y, N_XH, 2, 16, 512), "z", axis=0, tiled=False)

    held = sent_to_all(spread, PLANE)
    from_core = swapped(coeffs, "c")
    from_x = swapped(coeffs, "xl")
    from_both = swapped(from_x, "c")

    send = call(send_kernel, (N_Z, 2, 8, VEC), [SMEM, VMEM], 4, partner, held)
    arrived = lax.all_to_all(send, "z", 0, 0, tiled=True)
    kept = call(keep_kernel, (4, 64, VEC), [VMEM], 4, arrived)
    partners = lax.all_gather(kept, COL, axis=0, tiled=False)

    dens = call(
        density_kernel, (N_COL, 2, 2 * VEC, 512), [VMEM] + [HBM] * N_COL, 57,
        partners, isdf_coeffs, from_core, from_x, from_both, out=HBM,
        scratch=[
            pltpu.VMEM((N_COL, 2, 512, 256), jnp.bfloat16), pltpu.VMEM((N_COL, 2, 2 * VEC, 512), jnp.bfloat16),
            pltpu.SemaphoreType.DMA((N_COL,)), pltpu.SemaphoreType.DMA((N_COL,)),
        ],
    )
    projected = call(
        screen_kernel, (N_COL, 2, 64, VEC), [HBM] * 3, 60, rows, dens, isdf_coeffs,
        scratch=[
            pltpu.VMEM((N_COL, 2, N_Z, N_XH, 16, 512), jnp.bfloat16),
            pltpu.VMEM((N_COL, 2, 2 * VEC, 512), jnp.bfloat16), pltpu.VMEM((2, 512, 256), jnp.bfloat16),
            pltpu.SemaphoreType.DMA((N_COL, 2)), pltpu.SemaphoreType.DMA((N_COL, 2)), pltpu.SemaphoreType.DMA,
        ],
    )
    summed = lax.all_to_all(projected, COL, 0, 0, tiled=True).astype(jnp.float32).sum(axis=0)
    return summed + energies[:, :, None] * amps.astype(jnp.float32)


def solution(mesh):
    torus = Mesh(mesh.devices.reshape(N_Y, N_XH, N_Z, 2, 2), KA + COL)
    placed = (P(KA, COL, None), P(KA, COL, None), P(None, KA, COL), P(KA, COL), P(), P())
    return jax.shard_map(body, mesh=torus, in_specs=placed, out_specs=P(KA, COL, None), check_vma=False)
```

```python
import jax
import jax.numpy as jnp
from jax import lax
from jax.experimental import pallas as pl
from jax.experimental.pallas import tpu as pltpu
from jax.sharding import Mesh
from jax.sharding import PartitionSpec as P

KA = ("y", "xh", "z")
COL = ("xl", "c")
PLANE = ("y", "xh")
N_Y, N_XH, N_Z, N_COL = 4, 2, 16, 4
VEC = 192
SMEM = pl.BlockSpec(memory_space=pltpu.SMEM)
VMEM = pl.BlockSpec(memory_space=pltpu.VMEM)
HBM = pl.BlockSpec(memory_space=pltpu.HBM)


def slab_kernel(qsel, w, out, arrived):
    copies = [pltpu.make_async_copy(w.at[qsel[j]], out.at[j], arrived.at[j]) for j in range(2)]
    for copy in copies:
        copy.start()
    for copy in copies:
        copy.wait()


def paired(first, second):
    left = lax.broadcasted_iota(jnp.int32, first.shape, 1) < 64
    return jnp.where(left, first, second)


def pack_kernel(amps, out):
    for kl in range(2):
        out[kl * 64 : (kl + 1) * 64] = amps[kl, :, :128]
        out[128:, kl * 64 : (kl + 1) * 64] = amps[kl, :, 128:]


def send_kernel(partner, line, out):
    z = lax.axis_index("z")
    for yx in range(N_Y * N_XH):
        for j in range(2):
            ends = []
            for kl in range(2):
                wanted = partner[j, 2 * (yx * N_Z + z) + kl]
                row, side = (wanted >> 1) & 15, wanted & 1
                out[yx, j, kl * 64 : (kl + 1) * 64] = line[row, pl.ds(pl.multiple_of(side * 64, 64), 64)]
                end = line[row, 128:].astype(jnp.float32)
                ends.append(jnp.where(side == kl, end, pltpu.roll(end, 64, 1)))
            out[yx, j, 128:] = paired(*ends).astype(jnp.bfloat16)


def keep_kernel(partner, arrived, out):
    own = 2 * (lax.axis_index(PLANE) * N_Z + lax.axis_index("z"))
    for j in range(2):
        source = [partner[j, own + kl] >> 5 for kl in range(2)]
        for kl in range(2):
            out[j, kl * 64 : (kl + 1) * 64] = arrived[source[kl], j, kl * 64 : (kl + 1) * 64]
        ends = [arrived[at, j, 128:].astype(jnp.float32) for at in source]
        out[j, 128:] = paired(*ends).astype(jnp.bfloat16)


def by_z(block):
    rows = [block[(xh * N_Z + z) * 16 : (xh * N_Z + z + 1) * 16] for z in range(N_Z) for xh in range(N_XH)]
    return jnp.concatenate(rows, axis=0)


def density_kernel(partners, *refs):
    pieces, (out, coeffs, dens, arrived, written) = refs[:N_COL], refs[N_COL:]
    copies = [pltpu.make_async_copy(pieces[i], coeffs.at[i], arrived.at[i]) for i in range(N_COL)]
    stores = [pltpu.make_async_copy(dens.at[i], out.at[i], written.at[i]) for i in range(N_COL)]
    for copy in copies:
        copy.start()
    columns = []
    for slot in range(4):
        j, kl = divmod(slot, 2)
        own = slice(kl * 64, (kl + 1) * 64)
        whole = [
            jnp.concatenate(
                [partners[c, j, own].astype(jnp.float32), partners[c, j, 128:, own].astype(jnp.float32)], axis=1
            )
            for c in range(N_COL)
        ]
        columns.append(jnp.concatenate(whole, axis=0).T.astype(jnp.bfloat16))
    vectors = [jnp.concatenate([columns[kl], columns[2 + kl]], axis=0) for kl in range(2)]
    for i in range(N_COL):
        copies[i].wait()
        for kl in range(2):
            part = lax.dot_general(
                vectors[kl], by_z(coeffs[i, kl]), (((1,), (1,)), ((), ())), preferred_element_type=jnp.float32
            ).astype(jnp.bfloat16)
            dens[i, 0, kl * VEC : (kl + 1) * VEC, :] = part[:VEC]
            dens[i, 1, kl * VEC : (kl + 1) * VEC, :] = part[VEC:]
        stores[i].start()
    for store in stores:
        store.wait()


def screen_kernel(w, dens, own_coeffs, out, rows, held, coeffs, arrived, fetched, ready):
    c = lax.axis_index(COL)
    steps = [(j, i) for j in range(2) for i in range(N_COL)]
    copies = {(j, i): pltpu.make_async_copy(w.at[:, c ^ i, :, j], rows.at[i, j], arrived.at[i, j]) for j, i in steps}
    fetches = {(j, i): pltpu.make_async_copy(dens.at[i, j], held.at[i, j], fetched.at[i, j]) for j, i in steps}
    for step in steps:
        fetches[step].start()
        copies[step].start()
    last = pltpu.make_async_copy(own_coeffs, coeffs, ready)
    last.start()
    screened = []
    for j in range(2):
        total = None
        for i in range(N_COL):
            fetches[j, i].wait()
            copies[j, i].wait()
            part = jnp.dot(held[i, j], rows[i, j].reshape(512, 512), preferred_element_type=jnp.float32)
            total = part if total is None else total + part
        screened.append(total.astype(jnp.bfloat16))
    last.wait()
    for kl in range(2):
        own = slice(kl * VEC, (kl + 1) * VEC)
        projected = jnp.dot(screened[0][own], coeffs[kl], preferred_element_type=jnp.float32)
        projected += jnp.dot(screened[1][own], coeffs[kl], preferred_element_type=jnp.float32)
        result = projected.T.astype(jnp.bfloat16)
        for dest in range(N_COL):
            out[dest, kl] = result[dest * 64 : (dest + 1) * 64]


def swapped(array, axis):
    return lax.ppermute(array, axis, [(0, 1), (1, 0)])


def call(kernel, shape, specs, mib, *args, scratch=(), out=VMEM):
    return pl.pallas_call(
        kernel,
        out_shape=jax.ShapeDtypeStruct(shape, jnp.bfloat16),
        in_specs=specs,
        out_specs=out,
        scratch_shapes=scratch,
        compiler_params=pltpu.CompilerParams(vmem_limit_bytes=mib << 20),
    )(*args)


def sent_to_all(array, axis):
    length = lax.axis_size(axis)
    return lax.all_to_all(jnp.broadcast_to(array[None], (length, *array.shape)), axis, 0, 0, tiled=True)


def body(amps, isdf_coeffs, w_screen, energies, qsel, partner):
    slabs = call(
        slab_kernel, (2, 16, 512), [SMEM, HBM], 60, qsel, w_screen, scratch=[pltpu.SemaphoreType.DMA((2,))]
    )
    plane = sent_to_all(slabs, PLANE)
    plane, amps_, coeffs = lax.optimization_barrier((plane, amps, isdf_coeffs))
    rows = lax.all_gather(plane.reshape(N_Y, N_XH, 2, 16, 512), "z", axis=0, tiled=False)

    packed = call(pack_kernel, (192, 128), [VMEM], 4, amps_)
    line = lax.all_gather(packed, "z", axis=0, tiled=False)
    from_core = swapped(coeffs, "c")
    from_x = swapped(coeffs, "xl")
    from_both = swapped(from_x, "c")

    send = call(send_kernel, (8, 2, 192, 128), [SMEM, VMEM], 4, partner, line)
    arrived = lax.all_to_all(send, PLANE, 0, 0, tiled=True)
    kept = call(keep_kernel, (2, 192, 128), [SMEM, VMEM], 4, partner, arrived)
    partners = lax.all_gather(kept, COL, axis=0, tiled=False)

    dens = call(
        density_kernel, (N_COL, 2, 2 * VEC, 512), [VMEM] + [HBM] * N_COL, 57,
        partners, isdf_coeffs, from_core, from_x, from_both, out=HBM,
        scratch=[
            pltpu.VMEM((N_COL, 2, 512, 256), jnp.bfloat16), pltpu.VMEM((N_COL, 2, 2 * VEC, 512), jnp.bfloat16),
            pltpu.SemaphoreType.DMA((N_COL,)), pltpu.SemaphoreType.DMA((N_COL,)),
        ],
    )
    projected = call(
        screen_kernel, (N_COL, 2, 64, VEC), [HBM] * 3, 60, rows, dens, isdf_coeffs,
        scratch=[
            pltpu.VMEM((N_COL, 2, N_Z, N_XH, 16, 512), jnp.bfloat16),
            pltpu.VMEM((N_COL, 2, 2 * VEC, 512), jnp.bfloat16), pltpu.VMEM((2, 512, 256), jnp.bfloat16),
            pltpu.SemaphoreType.DMA((N_COL, 2)), pltpu.SemaphoreType.DMA((N_COL, 2)), pltpu.SemaphoreType.DMA,
        ],
    )
    summed = lax.all_to_all(projected, COL, 0, 0, tiled=True).astype(jnp.float32).sum(axis=0)
    return summed + energies[:, :, None] * amps.astype(jnp.float32)


def solution(mesh):
    torus = Mesh(mesh.devices.reshape(N_Y, N_XH, N_Z, 2, 2), KA + COL)
    placed = (P(KA, COL, None), P(KA, COL, None), P(None, KA, COL), P(KA, COL), P(), P())
    return jax.shard_map(body, mesh=torus, in_specs=placed, out_specs=P(KA, COL, None), check_vma=False)
```

```python
import jax
import jax.numpy as jnp
from jax import lax
from jax.experimental import pallas as pl
from jax.experimental.pallas import tpu as pltpu
from jax.sharding import Mesh
from jax.sharding import PartitionSpec as P

KA = ("y", "xh", "z")
COL = ("xl", "c")
PLANE = ("y", "xh")
N_Y, N_XH, N_Z, N_COL = 4, 2, 16, 4
VEC = 192
SMEM = pl.BlockSpec(memory_space=pltpu.SMEM)
VMEM = pl.BlockSpec(memory_space=pltpu.VMEM)
HBM = pl.BlockSpec(memory_space=pltpu.HBM)


def first_kernel(qsel, w, amps, slabs, packed, own, arrived, ready):
    fetch = pltpu.make_async_copy(amps, own, ready)
    fetch.start()
    copies = [
        pltpu.make_async_copy(w.at[qsel[j]], slabs.at[to, j], arrived.at[to, j])
        for to in range(N_Y * N_XH)
        for j in range(2)
    ]
    for copy in copies:
        copy.start()
    fetch.wait()
    for kl in range(2):
        packed[kl * 64 : (kl + 1) * 64] = own[kl, :, :128]
        packed[128:, kl * 64 : (kl + 1) * 64] = own[kl, :, 128:]
    for copy in copies:
        copy.wait()


def paired(first, second):
    left = lax.broadcasted_iota(jnp.int32, first.shape, 1) < 64
    return jnp.where(left, first, second)


def send_kernel(partner, line, out):
    z = lax.axis_index("z")
    for yx in range(N_Y * N_XH):
        for j in range(2):
            ends = []
            for kl in range(2):
                wanted = partner[j, 2 * (yx * N_Z + z) + kl]
                row, side = (wanted >> 1) & 15, wanted & 1
                out[yx, j, kl * 64 : (kl + 1) * 64] = line[row, pl.ds(pl.multiple_of(side * 64, 64), 64)]
                end = line[row, 128:].astype(jnp.float32)
                ends.append(jnp.where(side == kl, end, pltpu.roll(end, 64, 1)))
            out[yx, j, 128:] = paired(*ends).astype(jnp.bfloat16)


def keep_kernel(partner, arrived, out):
    own = 2 * (lax.axis_index(PLANE) * N_Z + lax.axis_index("z"))
    for j in range(2):
        source = [partner[j, own + kl] >> 5 for kl in range(2)]
        for kl in range(2):
            out[j, kl * 64 : (kl + 1) * 64] = arrived[source[kl], j, kl * 64 : (kl + 1) * 64]
        ends = [arrived[at, j, 128:].astype(jnp.float32) for at in source]
        out[j, 128:] = paired(*ends).astype(jnp.bfloat16)


def by_z(block):
    rows = [block[(xh * N_Z + z) * 16 : (xh * N_Z + z + 1) * 16] for z in range(N_Z) for xh in range(N_XH)]
    return jnp.concatenate(rows, axis=0)


def density_kernel(partners, *refs):
    pieces, (dens, coeffs, arrived) = refs[:N_COL], refs[N_COL:]
    copies = [pltpu.make_async_copy(pieces[i], coeffs.at[i], arrived.at[i]) for i in range(N_COL)]
    for copy in copies:
        copy.start()
    columns = []
    for slot in range(4):
        j, kl = divmod(slot, 2)
        own = slice(kl * 64, (kl + 1) * 64)
        whole = [
            jnp.concatenate(
                [partners[c, j, own].astype(jnp.float32), partners[c, j, 128:, own].astype(jnp.float32)], axis=1
            )
            for c in range(N_COL)
        ]
        columns.append(jnp.concatenate(whole, axis=0).T.astype(jnp.bfloat16))
    vectors = [jnp.concatenate([columns[kl], columns[2 + kl]], axis=0) for kl in range(2)]
    for i in range(N_COL):
        copies[i].wait()
        for kl in range(2):
            part = lax.dot_general(
                vectors[kl], by_z(coeffs[i, kl]), (((1,), (1,)), ((), ())), preferred_element_type=jnp.float32
            ).astype(jnp.bfloat16)
            dens[i, 0, kl * VEC : (kl + 1) * VEC, :] = part[:VEC]
            dens[i, 1, kl * VEC : (kl + 1) * VEC, :] = part[VEC:]


def screen_kernel(w, dens, own_coeffs, out, rows, coeffs, arrived, ready):
    c = lax.axis_index(COL)
    steps = [(j, i) for j in range(2) for i in range(N_COL)]
    copies = {(j, i): pltpu.make_async_copy(w.at[:, c ^ i, :, j], rows.at[i, j], arrived.at[i, j]) for j, i in steps}
    for step in steps:
        copies[step].start()
    last = pltpu.make_async_copy(own_coeffs, coeffs, ready)
    last.start()
    screened = []
    for j in range(2):
        total = None
        for i in range(N_COL):
            copies[j, i].wait()
            part = jnp.dot(dens[i, j], rows[i, j].reshape(512, 512), preferred_element_type=jnp.float32)
            total = part if total is None else total + part
        screened.append(total.astype(jnp.bfloat16))
    last.wait()
    for kl in range(2):
        own = slice(kl * VEC, (kl + 1) * VEC)
        projected = jnp.dot(screened[0][own], coeffs[kl], preferred_element_type=jnp.float32)
        projected += jnp.dot(screened[1][own], coeffs[kl], preferred_element_type=jnp.float32)
        result = projected.T.astype(jnp.bfloat16)
        for dest in range(N_COL):
            out[dest, kl * 64 : (kl + 1) * 64] = result[dest * 64 : (dest + 1) * 64, :128]
            out[dest, 128:, kl * 64 : (kl + 1) * 64] = result[dest * 64 : (dest + 1) * 64, 128:]


def last_kernel(arrived, base, out):
    total = sum(arrived[c].astype(jnp.float32) for c in range(N_COL))
    for kl in range(2):
        own = slice(kl * 64, (kl + 1) * 64)
        out[kl, :, :128] = base[kl, :, :128] + total[own]
        out[kl, :, 128:] = base[kl, :, 128:] + total[128:, own]


def swapped(array, axis):
    return lax.ppermute(array, axis, [(0, 1), (1, 0)])


def call(kernel, shape, specs, mib, *args, scratch=(), out=VMEM):
    return pl.pallas_call(
        kernel,
        out_shape=shape,
        in_specs=specs,
        out_specs=out,
        scratch_shapes=scratch,
        compiler_params=pltpu.CompilerParams(vmem_limit_bytes=mib << 20),
    )(*args)


def shaped(*shape, dtype=jnp.bfloat16):
    return jax.ShapeDtypeStruct(shape, dtype)


def in_hbm(array):
    return pltpu.with_memory_space_constraint(array, pltpu.HBM)


def sent_to_all(array, axis):
    length = lax.axis_size(axis)
    return lax.all_to_all(jnp.broadcast_to(array[None], (length, *array.shape)), axis, 0, 0, tiled=True)


def body(amps, isdf_coeffs, w_screen, energies, qsel, partner):
    slabs, packed = call(
        first_kernel, (shaped(8, 2, 16, 512), shaped(192, 128)), [SMEM, HBM, HBM], 4,
        qsel, in_hbm(w_screen), in_hbm(amps), out=(VMEM, VMEM),
        scratch=[
            pltpu.VMEM((2, 64, VEC), jnp.bfloat16), pltpu.SemaphoreType.DMA((8, 2)), pltpu.SemaphoreType.DMA,
        ],
    )
    plane = lax.all_to_all(slabs, PLANE, 0, 0, tiled=True)
    plane, packed, coeffs = lax.optimization_barrier((plane, packed, isdf_coeffs))
    rows = lax.all_gather(plane.reshape(N_Y, N_XH, 2, 16, 512), "z", axis=0, tiled=False)

    line = lax.all_gather(packed, "z", axis=0, tiled=False)
    from_core = swapped(coeffs, "c")
    from_x = swapped(coeffs, "xl")
    from_both = swapped(from_x, "c")

    send = call(send_kernel, shaped(8, 2, 192, 128), [SMEM, VMEM], 4, partner, line)
    arrived = lax.all_to_all(send, PLANE, 0, 0, tiled=True)
    kept = call(keep_kernel, shaped(2, 192, 128), [SMEM, VMEM], 4, partner, arrived)
    partners = lax.all_gather(kept, COL, axis=0, tiled=False)

    dens = call(
        density_kernel, shaped(N_COL, 2, 2 * VEC, 512), [VMEM] + [HBM] * N_COL, 24,
        partners, *(in_hbm(piece) for piece in (isdf_coeffs, from_core, from_x, from_both)),
        scratch=[pltpu.VMEM((N_COL, 2, 512, 256), jnp.bfloat16), pltpu.SemaphoreType.DMA((N_COL,))],
    )
    projected = call(
        screen_kernel, shaped(N_COL, 192, 128), [HBM, VMEM, HBM], 24, in_hbm(rows), dens, in_hbm(isdf_coeffs),
        scratch=[
            pltpu.VMEM((N_COL, 2, N_Z, N_XH, 16, 512), jnp.bfloat16), pltpu.VMEM((2, 512, 256), jnp.bfloat16),
            pltpu.SemaphoreType.DMA((N_COL, 2)), pltpu.SemaphoreType.DMA,
        ],
    )
    base = energies[:, :, None] * amps.astype(jnp.float32)
    summed = lax.all_to_all(projected, COL, 0, 0, tiled=True)
    return call(last_kernel, shaped(2, 64, VEC, dtype=jnp.float32), [VMEM, VMEM], 4, summed, base)


def solution(mesh):
    torus = Mesh(mesh.devices.reshape(N_Y, N_XH, N_Z, 2, 2), KA + COL)
    placed = (P(KA, COL, None), P(KA, COL, None), P(None, KA, COL), P(KA, COL), P(), P())
    return jax.shard_map(body, mesh=torus, in_specs=placed, out_specs=P(KA, COL, None), check_vma=False)
```

```python
import jax
import jax.numpy as jnp
from jax import lax
from jax.experimental import pallas as pl
from jax.experimental.pallas import tpu as pltpu
from jax.sharding import Mesh
from jax.sharding import PartitionSpec as P

KA = ("y", "xh", "z")
COL = ("xl", "c")
PLANE = ("y", "xh")
N_Y, N_XH, N_Z, N_COL = 4, 2, 16, 4
VEC = 192
SMEM = pl.BlockSpec(memory_space=pltpu.SMEM)
VMEM = pl.BlockSpec(memory_space=pltpu.VMEM)
HBM = pl.BlockSpec(memory_space=pltpu.HBM)


def first_kernel(qsel, w, amps, slabs, packed, own, arrived, ready):
    fetch = pltpu.make_async_copy(amps, own, ready)
    fetch.start()
    copies = [
        pltpu.make_async_copy(w.at[qsel[j]], slabs.at[to, j], arrived.at[to, j])
        for to in range(N_Y * N_XH)
        for j in range(2)
    ]
    for copy in copies:
        copy.start()
    fetch.wait()
    for kl in range(2):
        packed[kl * 64 : (kl + 1) * 64] = own[kl, :, :128]
        packed[128:, kl * 64 : (kl + 1) * 64] = own[kl, :, 128:]
    for copy in copies:
        copy.wait()


def paired(first, second):
    left = lax.broadcasted_iota(jnp.int32, first.shape, 1) < 64
    return jnp.where(left, first, second)


def send_kernel(partner, line, out):
    z = lax.axis_index("z")
    for yx in range(N_Y * N_XH):
        for j in range(2):
            ends = []
            for kl in range(2):
                wanted = partner[j, 2 * (yx * N_Z + z) + kl]
                row, side = (wanted >> 1) & 15, wanted & 1
                out[yx, j, kl * 64 : (kl + 1) * 64] = line[row, pl.ds(pl.multiple_of(side * 64, 64), 64)]
                end = line[row, 128:].astype(jnp.float32)
                ends.append(jnp.where(side == kl, end, pltpu.roll(end, 64, 1)))
            out[yx, j, 128:] = paired(*ends).astype(jnp.bfloat16)


def keep_kernel(partner, arrived, out):
    own = 2 * (lax.axis_index(PLANE) * N_Z + lax.axis_index("z"))
    for j in range(2):
        source = [partner[j, own + kl] >> 5 for kl in range(2)]
        for kl in range(2):
            out[j, kl * 64 : (kl + 1) * 64] = arrived[source[kl], j, kl * 64 : (kl + 1) * 64]
        ends = [arrived[at, j, 128:].astype(jnp.float32) for at in source]
        out[j, 128:] = paired(*ends).astype(jnp.bfloat16)


def by_z(block):
    rows = [block[(xh * N_Z + z) * 16 : (xh * N_Z + z + 1) * 16] for z in range(N_Z) for xh in range(N_XH)]
    return jnp.concatenate(rows, axis=0)


def density_kernel(partners, *refs):
    pieces, (dens, coeffs, arrived) = refs[:N_COL], refs[N_COL:]
    copies = [pltpu.make_async_copy(pieces[i], coeffs.at[i], arrived.at[i]) for i in range(N_COL)]
    for copy in copies:
        copy.start()
    columns = []
    for slot in range(4):
        j, kl = divmod(slot, 2)
        own = slice(kl * 64, (kl + 1) * 64)
        whole = [
            jnp.concatenate(
                [partners[c, j, own].astype(jnp.float32), partners[c, j, 128:, own].astype(jnp.float32)], axis=1
            )
            for c in range(N_COL)
        ]
        columns.append(jnp.concatenate(whole, axis=0).T.astype(jnp.bfloat16))
    vectors = [jnp.concatenate([columns[kl], columns[2 + kl]], axis=0) for kl in range(2)]
    for i in range(N_COL):
        copies[i].wait()
        for kl in range(2):
            part = lax.dot_general(
                vectors[kl], by_z(coeffs[i, kl]), (((1,), (1,)), ((), ())), preferred_element_type=jnp.float32
            ).astype(jnp.bfloat16)
            dens[i, 0, kl * VEC : (kl + 1) * VEC, :] = part[:VEC]
            dens[i, 1, kl * VEC : (kl + 1) * VEC, :] = part[VEC:]


def screen_kernel(w, dens, own_coeffs, out, rows, coeffs, arrived, ready):
    c = lax.axis_index(COL)
    steps = [(j, i) for j in range(2) for i in range(N_COL)]
    copies = {(j, i): pltpu.make_async_copy(w.at[:, c ^ i, :, j], rows.at[i, j], arrived.at[i, j]) for j, i in steps}
    for step in steps:
        copies[step].start()
    last = pltpu.make_async_copy(own_coeffs, coeffs, ready)
    last.start()
    screened = []
    for j in range(2):
        total = None
        for i in range(N_COL):
            copies[j, i].wait()
            part = jnp.dot(dens[i, j], rows[i, j].reshape(512, 512), preferred_element_type=jnp.float32)
            total = part if total is None else total + part
        screened.append(total.astype(jnp.bfloat16))
    last.wait()
    for kl in range(2):
        own = slice(kl * VEC, (kl + 1) * VEC)
        projected = jnp.dot(screened[0][own], coeffs[kl], preferred_element_type=jnp.float32)
        projected += jnp.dot(screened[1][own], coeffs[kl], preferred_element_type=jnp.float32)
        result = projected.T.astype(jnp.bfloat16)
        for dest in range(N_COL):
            out[dest, kl * 64 : (kl + 1) * 64] = result[dest * 64 : (dest + 1) * 64, :128]
            out[dest, 128:, kl * 64 : (kl + 1) * 64] = result[dest * 64 : (dest + 1) * 64, 128:]


def last_kernel(arrived, base, out):
    total = sum(arrived[c].astype(jnp.float32) for c in range(N_COL))
    for kl in range(2):
        own = slice(kl * 64, (kl + 1) * 64)
        out[kl, :, :128] = base[kl, :, :128] + total[own]
        out[kl, :, 128:] = base[kl, :, 128:] + total[128:, own]


def swapped(array, axis):
    return lax.ppermute(array, axis, [(0, 1), (1, 0)])


def call(kernel, shape, specs, mib, *args, scratch=(), out=VMEM):
    return pl.pallas_call(
        kernel,
        out_shape=shape,
        in_specs=specs,
        out_specs=out,
        scratch_shapes=scratch,
        compiler_params=pltpu.CompilerParams(vmem_limit_bytes=mib << 20),
    )(*args)


def shaped(*shape, dtype=jnp.bfloat16):
    return jax.ShapeDtypeStruct(shape, dtype)


def in_hbm(array):
    return pltpu.with_memory_space_constraint(array, pltpu.HBM)


def sent_to_all(array, axis):
    length = lax.axis_size(axis)
    return lax.all_to_all(jnp.broadcast_to(array[None], (length, *array.shape)), axis, 0, 0, tiled=True)


def body(amps, isdf_coeffs, w_screen, energies, qsel, partner):
    slabs, packed = call(
        first_kernel, (shaped(8, 2, 16, 512), shaped(192, 128)), [SMEM, HBM, HBM], 4,
        in_hbm(qsel), in_hbm(w_screen), in_hbm(amps), out=(VMEM, VMEM),
        scratch=[
            pltpu.VMEM((2, 64, VEC), jnp.bfloat16), pltpu.SemaphoreType.DMA((8, 2)), pltpu.SemaphoreType.DMA,
        ],
    )
    plane = lax.all_to_all(slabs, PLANE, 0, 0, tiled=True)
    plane, packed, coeffs = lax.optimization_barrier((plane, packed, isdf_coeffs))
    rows = lax.all_gather(plane.reshape(N_Y, N_XH, 2, 16, 512), "z", axis=0, tiled=False)

    line = lax.all_gather(packed, "z", axis=0, tiled=False)
    from_core = swapped(coeffs, "c")
    from_x = swapped(coeffs, "xl")
    from_both = swapped(from_x, "c")

    send = call(send_kernel, pltpu.VMEM((8, 2, 192, 128), jnp.bfloat16), [SMEM, VMEM], 4, in_hbm(partner), line)
    arrived = lax.all_to_all(send, PLANE, 0, 0, tiled=True)
    kept = call(keep_kernel, shaped(2, 192, 128), [SMEM, VMEM], 4, in_hbm(partner), arrived)
    partners = lax.all_gather(kept, COL, axis=0, tiled=False)

    dens = call(
        density_kernel, shaped(N_COL, 2, 2 * VEC, 512), [VMEM] + [HBM] * N_COL, 24,
        partners, *(in_hbm(piece) for piece in (isdf_coeffs, from_core, from_x, from_both)),
        scratch=[pltpu.VMEM((N_COL, 2, 512, 256), jnp.bfloat16), pltpu.SemaphoreType.DMA((N_COL,))],
    )
    base = energies[:, :, None] * amps.astype(jnp.float32)
    dens, base = lax.optimization_barrier((dens, base))
    projected = call(
        screen_kernel, pltpu.VMEM((N_COL, 192, 128), jnp.bfloat16), [HBM, VMEM, HBM], 24, in_hbm(rows), dens, in_hbm(isdf_coeffs),
        scratch=[
            pltpu.VMEM((N_COL, 2, N_Z, N_XH, 16, 512), jnp.bfloat16), pltpu.VMEM((2, 512, 256), jnp.bfloat16),
            pltpu.SemaphoreType.DMA((N_COL, 2)), pltpu.SemaphoreType.DMA,
        ],
    )
    summed = lax.all_to_all(projected, COL, 0, 0, tiled=True)
    return call(last_kernel, shaped(2, 64, VEC, dtype=jnp.float32), [VMEM, VMEM], 4, summed, base)


def solution(mesh):
    torus = Mesh(mesh.devices.reshape(N_Y, N_XH, N_Z, 2, 2), KA + COL)
    placed = (P(KA, COL, None), P(KA, COL, None), P(None, KA, COL), P(KA, COL), P(), P())
    return jax.shard_map(body, mesh=torus, in_specs=placed, out_specs=P(KA, COL, None), check_vma=False)
```

```python
import jax
import jax.numpy as jnp
from jax import lax
from jax.experimental import pallas as pl
from jax.experimental.pallas import tpu as pltpu
from jax.sharding import Mesh
from jax.sharding import PartitionSpec as P

KA = ("y", "xh", "z")
COL = ("xl", "c")
PLANE = ("y", "xh")
N_Y, N_XH, N_Z, N_COL = 4, 2, 16, 4
VEC = 192
SMEM = pl.BlockSpec(memory_space=pltpu.SMEM)
VMEM = pl.BlockSpec(memory_space=pltpu.VMEM)
HBM = pl.BlockSpec(memory_space=pltpu.HBM)


def first_kernel(qsel, w, amps, slabs, packed, own, arrived, ready):
    fetch = pltpu.make_async_copy(amps, own, ready)
    fetch.start()
    copies = [
        pltpu.make_async_copy(w.at[qsel[j]], slabs.at[to, j], arrived.at[to, j])
        for to in range(N_Y * N_XH)
        for j in range(2)
    ]
    for copy in copies:
        copy.start()
    fetch.wait()
    for kl in range(2):
        packed[kl * 64 : (kl + 1) * 64] = own[kl, :, :128]
        packed[128:, kl * 64 : (kl + 1) * 64] = own[kl, :, 128:]
    for copy in copies:
        copy.wait()


def paired(first, second):
    left = lax.broadcasted_iota(jnp.int32, first.shape, 1) < 64
    return jnp.where(left, first, second)


def send_kernel(partner, line, out):
    z = lax.axis_index("z")
    for yx in range(N_Y * N_XH):
        for j in range(2):
            ends = []
            for kl in range(2):
                wanted = partner[j, 2 * (yx * N_Z + z) + kl]
                row, side = (wanted >> 1) & 15, wanted & 1
                out[yx, j, kl * 64 : (kl + 1) * 64] = line[row, pl.ds(pl.multiple_of(side * 64, 64), 64)]
                end = line[row, 128:].astype(jnp.float32)
                ends.append(jnp.where(side == kl, end, pltpu.roll(end, 64, 1)))
            out[yx, j, 128:] = paired(*ends).astype(jnp.bfloat16)


def keep_kernel(partner, arrived, out):
    own = 2 * (lax.axis_index(PLANE) * N_Z + lax.axis_index("z"))
    for j in range(2):
        source = [partner[j, own + kl] >> 5 for kl in range(2)]
        for kl in range(2):
            out[j, kl * 64 : (kl + 1) * 64] = arrived[source[kl], j, kl * 64 : (kl + 1) * 64]
        ends = [arrived[at, j, 128:].astype(jnp.float32) for at in source]
        out[j, 128:] = paired(*ends).astype(jnp.bfloat16)


def by_z(block):
    rows = [block[(xh * N_Z + z) * 16 : (xh * N_Z + z + 1) * 16] for z in range(N_Z) for xh in range(N_XH)]
    return jnp.concatenate(rows, axis=0)


def density_kernel(partners, *refs):
    pieces, (dens, coeffs, arrived) = refs[:N_COL], refs[N_COL:]
    copies = [pltpu.make_async_copy(pieces[i], coeffs.at[i], arrived.at[i]) for i in range(N_COL)]
    for copy in copies:
        copy.start()
    columns = []
    for slot in range(4):
        j, kl = divmod(slot, 2)
        own = slice(kl * 64, (kl + 1) * 64)
        whole = [
            jnp.concatenate(
                [partners[c, j, own].astype(jnp.float32), partners[c, j, 128:, own].astype(jnp.float32)], axis=1
            )
            for c in range(N_COL)
        ]
        columns.append(jnp.concatenate(whole, axis=0).T.astype(jnp.bfloat16))
    vectors = [jnp.concatenate([columns[kl], columns[2 + kl]], axis=0) for kl in range(2)]
    for i in range(N_COL):
        copies[i].wait()
        for kl in range(2):
            part = lax.dot_general(
                vectors[kl], by_z(coeffs[i, kl]), (((1,), (1,)), ((), ())), preferred_element_type=jnp.float32
            ).astype(jnp.bfloat16)
            dens[i, 0, kl * VEC : (kl + 1) * VEC, :] = part[:VEC]
            dens[i, 1, kl * VEC : (kl + 1) * VEC, :] = part[VEC:]


def screen_kernel(w, dens, own_coeffs, out, rows, coeffs, arrived, ready):
    c = lax.axis_index(COL)
    steps = [(j, i) for j in range(2) for i in range(N_COL)]
    copies = {(j, i): pltpu.make_async_copy(w.at[:, c ^ i, :, j], rows.at[i, j], arrived.at[i, j]) for j, i in steps}
    for step in steps:
        copies[step].start()
    last = pltpu.make_async_copy(own_coeffs, coeffs, ready)
    last.start()
    screened = []
    for j in range(2):
        total = None
        for i in range(N_COL):
            copies[j, i].wait()
            part = jnp.dot(dens[i, j], rows[i, j].reshape(512, 512), preferred_element_type=jnp.float32)
            total = part if total is None else total + part
        screened.append(total.astype(jnp.bfloat16))
    last.wait()
    for kl in range(2):
        own = slice(kl * VEC, (kl + 1) * VEC)
        projected = jnp.dot(screened[0][own], coeffs[kl], preferred_element_type=jnp.float32)
        projected += jnp.dot(screened[1][own], coeffs[kl], preferred_element_type=jnp.float32)
        result = projected.T.astype(jnp.bfloat16)
        for dest in range(N_COL):
            out[dest, kl * 64 : (kl + 1) * 64] = result[dest * 64 : (dest + 1) * 64, :128]
            out[dest, 128:, kl * 64 : (kl + 1) * 64] = result[dest * 64 : (dest + 1) * 64, 128:]


def last_kernel(arrived, base, out):
    total = sum(arrived[c].astype(jnp.float32) for c in range(N_COL))
    for kl in range(2):
        own = slice(kl * 64, (kl + 1) * 64)
        out[kl, :, :128] = base[kl, :, :128] + total[own]
        out[kl, :, 128:] = base[kl, :, 128:] + total[128:, own]


def swapped(array, axis):
    return lax.ppermute(array, axis, [(0, 1), (1, 0)])


def call(kernel, shape, specs, mib, *args, scratch=(), out=VMEM):
    return pl.pallas_call(
        kernel,
        out_shape=shape,
        in_specs=specs,
        out_specs=out,
        scratch_shapes=scratch,
        compiler_params=pltpu.CompilerParams(vmem_limit_bytes=mib << 20),
    )(*args)


def shaped(*shape, dtype=jnp.bfloat16):
    return jax.ShapeDtypeStruct(shape, dtype)


def in_hbm(array):
    return pltpu.with_memory_space_constraint(array, pltpu.HBM)


def sent_to_all(array, axis):
    length = lax.axis_size(axis)
    return lax.all_to_all(jnp.broadcast_to(array[None], (length, *array.shape)), axis, 0, 0, tiled=True)


def body(amps, isdf_coeffs, w_screen, energies, qsel, partner):
    slabs, packed = call(
        first_kernel, (shaped(8, 2, 16, 512), shaped(192, 128)), [SMEM, HBM, HBM], 4,
        in_hbm(qsel), in_hbm(w_screen), in_hbm(amps), out=(VMEM, VMEM),
        scratch=[
            pltpu.VMEM((2, 64, VEC), jnp.bfloat16), pltpu.SemaphoreType.DMA((8, 2)), pltpu.SemaphoreType.DMA,
        ],
    )
    plane = lax.all_to_all(slabs, PLANE, 0, 0, tiled=True)
    plane, packed = lax.optimization_barrier((plane, packed))
    rows = lax.all_gather(plane.reshape(N_Y, N_XH, 2, 16, 512), "z", axis=0, tiled=False)

    line = lax.all_gather(packed, "z", axis=0, tiled=False)
    line, coeffs = lax.optimization_barrier((line, isdf_coeffs))
    from_core = swapped(coeffs, "c")
    from_x = swapped(coeffs, "xl")
    from_both = swapped(from_x, "c")

    send = call(send_kernel, pltpu.VMEM((8, 2, 192, 128), jnp.bfloat16), [SMEM, VMEM], 4, in_hbm(partner), line)
    arrived = lax.all_to_all(send, PLANE, 0, 0, tiled=True)
    kept = call(keep_kernel, shaped(2, 192, 128), [SMEM, VMEM], 4, in_hbm(partner), arrived)
    partners = lax.all_gather(kept, COL, axis=0, tiled=False)

    dens = call(
        density_kernel, shaped(N_COL, 2, 2 * VEC, 512), [VMEM] + [HBM] * N_COL, 24,
        partners, *(in_hbm(piece) for piece in (isdf_coeffs, from_core, from_x, from_both)),
        scratch=[pltpu.VMEM((N_COL, 2, 512, 256), jnp.bfloat16), pltpu.SemaphoreType.DMA((N_COL,))],
    )
    base = energies[:, :, None] * amps.astype(jnp.float32)
    dens, base = lax.optimization_barrier((dens, base))
    projected = call(
        screen_kernel, pltpu.VMEM((N_COL, 192, 128), jnp.bfloat16), [HBM, VMEM, HBM], 24, in_hbm(rows), dens, in_hbm(isdf_coeffs),
        scratch=[
            pltpu.VMEM((N_COL, 2, N_Z, N_XH, 16, 512), jnp.bfloat16), pltpu.VMEM((2, 512, 256), jnp.bfloat16),
            pltpu.SemaphoreType.DMA((N_COL, 2)), pltpu.SemaphoreType.DMA,
        ],
    )
    summed = lax.all_to_all(projected, COL, 0, 0, tiled=True)
    return call(last_kernel, shaped(2, 64, VEC, dtype=jnp.float32), [VMEM, VMEM], 4, summed, base)


def solution(mesh):
    torus = Mesh(mesh.devices.reshape(N_Y, N_XH, N_Z, 2, 2), KA + COL)
    placed = (P(KA, COL, None), P(KA, COL, None), P(None, KA, COL), P(KA, COL), P(), P())
    return jax.shard_map(body, mesh=torus, in_specs=placed, out_specs=P(KA, COL, None), check_vma=False)
```

```python
import jax
import jax.numpy as jnp
from jax import lax
from jax.experimental import pallas as pl
from jax.experimental.pallas import tpu as pltpu
from jax.sharding import Mesh
from jax.sharding import PartitionSpec as P

KA = ("y", "xh", "z")
COL = ("xl", "c")
PLANE = ("y", "xh")
N_Y, N_XH, N_Z, N_COL = 4, 2, 16, 4
VEC = 192
SMEM = pl.BlockSpec(memory_space=pltpu.SMEM)
VMEM = pl.BlockSpec(memory_space=pltpu.VMEM)
HBM = pl.BlockSpec(memory_space=pltpu.HBM)


def first_kernel(qsel, w, amps, slabs, packed, own, arrived, ready):
    fetch = pltpu.make_async_copy(amps, own, ready)
    fetch.start()
    copies = [
        pltpu.make_async_copy(w.at[qsel[j]], slabs.at[to, j], arrived.at[to, j])
        for to in range(N_Y * N_XH)
        for j in range(2)
    ]
    for copy in copies:
        copy.start()
    fetch.wait()
    for kl in range(2):
        packed[kl * 64 : (kl + 1) * 64] = own[kl, :, :128]
        packed[128:, kl * 64 : (kl + 1) * 64] = own[kl, :, 128:]
    for copy in copies:
        copy.wait()


def paired(first, second):
    left = lax.broadcasted_iota(jnp.int32, first.shape, 1) < 64
    return jnp.where(left, first, second)


def send_kernel(partner, line, out):
    z = lax.axis_index("z")
    for yx in range(N_Y * N_XH):
        for j in range(2):
            ends = []
            for kl in range(2):
                wanted = partner[j, 2 * (yx * N_Z + z) + kl]
                row, side = (wanted >> 1) & 15, wanted & 1
                out[yx, j, kl * 64 : (kl + 1) * 64] = line[row, pl.ds(pl.multiple_of(side * 64, 64), 64)]
                end = line[row, 128:].astype(jnp.float32)
                ends.append(jnp.where(side == kl, end, pltpu.roll(end, 64, 1)))
            out[yx, j, 128:] = paired(*ends).astype(jnp.bfloat16)


def keep_kernel(partner, arrived, out):
    own = 2 * (lax.axis_index(PLANE) * N_Z + lax.axis_index("z"))
    for j in range(2):
        source = [partner[j, own + kl] >> 5 for kl in range(2)]
        for kl in range(2):
            out[j, kl * 64 : (kl + 1) * 64] = arrived[source[kl], j, kl * 64 : (kl + 1) * 64]
        ends = [arrived[at, j, 128:].astype(jnp.float32) for at in source]
        out[j, 128:] = paired(*ends).astype(jnp.bfloat16)


def by_z(block):
    rows = [block[(xh * N_Z + z) * 16 : (xh * N_Z + z + 1) * 16] for z in range(N_Z) for xh in range(N_XH)]
    return jnp.concatenate(rows, axis=0)


def density_kernel(partners, *refs):
    pieces, (dens, coeffs, arrived) = refs[:N_COL], refs[N_COL:]
    copies = [pltpu.make_async_copy(pieces[i], coeffs.at[i], arrived.at[i]) for i in range(N_COL)]
    for copy in copies:
        copy.start()
    columns = []
    for slot in range(4):
        j, kl = divmod(slot, 2)
        own = slice(kl * 64, (kl + 1) * 64)
        whole = [
            jnp.concatenate(
                [partners[c, j, own].astype(jnp.float32), partners[c, j, 128:, own].astype(jnp.float32)], axis=1
            )
            for c in range(N_COL)
        ]
        columns.append(jnp.concatenate(whole, axis=0).T.astype(jnp.bfloat16))
    vectors = [jnp.concatenate([columns[kl], columns[2 + kl]], axis=0) for kl in range(2)]
    for i in range(N_COL):
        copies[i].wait()
        for kl in range(2):
            part = lax.dot_general(
                vectors[kl], by_z(coeffs[i, kl]), (((1,), (1,)), ((), ())), preferred_element_type=jnp.float32
            ).astype(jnp.bfloat16)
            dens[i, 0, kl * VEC : (kl + 1) * VEC, :] = part[:VEC]
            dens[i, 1, kl * VEC : (kl + 1) * VEC, :] = part[VEC:]


def screen_kernel(w, dens, own_coeffs, out, rows, coeffs, arrived, ready):
    c = lax.axis_index(COL)
    steps = [(j, i) for j in range(2) for i in range(N_COL)]
    copies = {(j, i): pltpu.make_async_copy(w.at[:, :, c ^ i, j], rows.at[i, j], arrived.at[i, j]) for j, i in steps}
    for step in steps:
        copies[step].start()
    last = pltpu.make_async_copy(own_coeffs, coeffs, ready)
    last.start()
    screened = []
    for j in range(2):
        total = None
        for i in range(N_COL):
            copies[j, i].wait()
            part = jnp.dot(dens[i, j], rows[i, j].reshape(512, 512), preferred_element_type=jnp.float32)
            total = part if total is None else total + part
        screened.append(total.astype(jnp.bfloat16))
    last.wait()
    for kl in range(2):
        own = slice(kl * VEC, (kl + 1) * VEC)
        projected = jnp.dot(screened[0][own], coeffs[kl], preferred_element_type=jnp.float32)
        projected += jnp.dot(screened[1][own], coeffs[kl], preferred_element_type=jnp.float32)
        result = projected.T.astype(jnp.bfloat16)
        for dest in range(N_COL):
            out[dest, kl * 64 : (kl + 1) * 64] = result[dest * 64 : (dest + 1) * 64, :128]
            out[dest, 128:, kl * 64 : (kl + 1) * 64] = result[dest * 64 : (dest + 1) * 64, 128:]


def last_kernel(arrived, base, out):
    total = sum(arrived[c].astype(jnp.float32) for c in range(N_COL))
    for kl in range(2):
        own = slice(kl * 64, (kl + 1) * 64)
        out[kl, :, :128] = base[kl, :, :128] + total[own]
        out[kl, :, 128:] = base[kl, :, 128:] + total[128:, own]


def swapped(array, axis):
    return lax.ppermute(array, axis, [(0, 1), (1, 0)])


def call(kernel, shape, specs, mib, *args, scratch=(), out=VMEM):
    return pl.pallas_call(
        kernel,
        out_shape=shape,
        in_specs=specs,
        out_specs=out,
        scratch_shapes=scratch,
        compiler_params=pltpu.CompilerParams(vmem_limit_bytes=mib << 20),
    )(*args)


def shaped(*shape, dtype=jnp.bfloat16):
    return jax.ShapeDtypeStruct(shape, dtype)


def in_hbm(array):
    return pltpu.with_memory_space_constraint(array, pltpu.HBM)


def sent_to_all(array, axis):
    length = lax.axis_size(axis)
    return lax.all_to_all(jnp.broadcast_to(array[None], (length, *array.shape)), axis, 0, 0, tiled=True)


def body(amps, isdf_coeffs, w_screen, energies, qsel, partner):
    slabs, packed = call(
        first_kernel, (shaped(8, 2, 16, 512), shaped(192, 128)), [SMEM, HBM, HBM], 4,
        in_hbm(qsel), in_hbm(w_screen), in_hbm(amps), out=(VMEM, VMEM),
        scratch=[
            pltpu.VMEM((2, 64, VEC), jnp.bfloat16), pltpu.SemaphoreType.DMA((8, 2)), pltpu.SemaphoreType.DMA,
        ],
    )
    plane = lax.all_to_all(slabs, ("xh", "y"), 0, 0, tiled=True)
    plane, packed = lax.optimization_barrier((plane, packed))
    rows = lax.all_gather(plane.reshape(N_XH, N_Y, 2, 16, 512), "z", axis=0, tiled=False)

    line = lax.all_gather(packed, "z", axis=0, tiled=False)
    line, coeffs = lax.optimization_barrier((line, isdf_coeffs))
    from_core = swapped(coeffs, "c")
    from_x = swapped(coeffs, "xl")
    from_both = swapped(from_x, "c")

    send = call(send_kernel, pltpu.VMEM((8, 2, 192, 128), jnp.bfloat16), [SMEM, VMEM], 4, in_hbm(partner), line)
    arrived = lax.all_to_all(send, PLANE, 0, 0, tiled=True)
    kept = call(keep_kernel, shaped(2, 192, 128), [SMEM, VMEM], 4, in_hbm(partner), arrived)
    partners = lax.all_gather(kept, COL, axis=0, tiled=False)

    dens = call(
        density_kernel, shaped(N_COL, 2, 2 * VEC, 512), [VMEM] + [HBM] * N_COL, 24,
        partners, *(in_hbm(piece) for piece in (isdf_coeffs, from_core, from_x, from_both)),
        scratch=[pltpu.VMEM((N_COL, 2, 512, 256), jnp.bfloat16), pltpu.SemaphoreType.DMA((N_COL,))],
    )
    base = energies[:, :, None] * amps.astype(jnp.float32)
    dens, base = lax.optimization_barrier((dens, base))
    projected = call(
        screen_kernel, pltpu.VMEM((N_COL, 192, 128), jnp.bfloat16), [HBM, VMEM, HBM], 24, in_hbm(rows), dens, in_hbm(isdf_coeffs),
        scratch=[
            pltpu.VMEM((N_COL, 2, N_Z, N_XH, 16, 512), jnp.bfloat16), pltpu.VMEM((2, 512, 256), jnp.bfloat16),
            pltpu.SemaphoreType.DMA((N_COL, 2)), pltpu.SemaphoreType.DMA,
        ],
    )
    summed = lax.all_to_all(projected, COL, 0, 0, tiled=True)
    return call(last_kernel, shaped(2, 64, VEC, dtype=jnp.float32), [VMEM, VMEM], 4, summed, base)


def solution(mesh):
    torus = Mesh(mesh.devices.reshape(N_Y, N_XH, N_Z, 2, 2), KA + COL)
    placed = (P(KA, COL, None), P(KA, COL, None), P(None, KA, COL), P(KA, COL), P(), P())
    return jax.shard_map(body, mesh=torus, in_specs=placed, out_specs=P(KA, COL, None), check_vma=False)
```
